32 devices in a mesh: gx: 4 (over y, x), gy: 4 (over z), gz: 2 (over core).
Axes of the slice: x: 2, y: 2, z: 4, core: 2. Of those that a mesh axis runs over, the one named last changes fastest.
Arguments:
- residual_in: float32 [2, 4, 64, 64, 256], P(None, None, 'gx', 'gy', 'gz'), may hold values from -15 to 15
- reaction: float32 [4, 64, 64, 256], P(None, 'gx', 'gy', 'gz'), may hold values from 0.5 to 2
- transport: float32 [4, 64, 64, 256], P(None, 'gx', 'gy', 'gz'), may hold values from 0.2 to 1
- congestion: float32 [4, 64, 64, 256], P(None, 'gx', 'gy', 'gz'), may hold values from 0.5 to 1.5
Outputs:
- newton_update: float32 [2, 4, 64, 64, 256], P(None, None, 'gx', 'gy', 'gz')
The draws below stay inside these ranges and needn't reach their ends.
All inputs are finite; a program needn't handle non-finite values.
Results may differ from the reference program's by a relative error of at most 0.0003.
Values sent between devices are 32-bit elements; how exact they have to be, the bound alone decides.
A program may use at most 128 MiB of HBM per device.

```python
import jax
import jax.numpy as jnp

LEVELS = 4
ITERS = 8
NX = 64
NY = 64
NZ = 256


def level_of(own_key, shape, cuts, low, top_value):
    factor_of = 1.0
    for dim, blocks in cuts:
        draws = jax.random.uniform(jax.random.fold_in(jax.random.fold_in(own_key, 6), dim), (blocks,), jnp.float32, low / len(cuts), top_value / len(cuts))
        factor_of = factor_of * jnp.repeat(jnp.exp(draws), shape[dim] // blocks).reshape((-1,) + (1,) * (len(shape) - 1 - dim))
    return factor_of


def normal_values(rng, extent, scale, bound, pieces=(), held_as=jnp.bfloat16):
    drawn = jax.random.normal(rng, extent, jnp.float32) * scale
    if len(pieces) > 0:
        drawn = level_of(rng, extent, pieces, -0.22, 0.18) * drawn
    return jnp.clip(drawn, min=-bound, max=bound).astype(held_as)


def setup_inputs(seed: int = 0) -> dict:
    seeds = jax.random.split(jax.random.key(seed), 5)
    return {
        "residual_in": normal_values(seeds[0], (2, LEVELS, NX, NY, NZ), 3.0, 15.0, ((2, 4), (3, 4), (4, 2)), jnp.float32),
        "reaction": jnp.clip(0.5 + 1.5 * jax.random.uniform(seeds[1], (LEVELS, NX, NY, NZ), jnp.float32) ** level_of(seeds[1], (LEVELS, NX, NY, NZ), ((1, 4), (2, 4), (3, 2)), -0.2, 0.2), 0.5, 2.0),
        "transport": jnp.clip(0.2 + 0.8 * jax.random.uniform(seeds[2], (LEVELS, NX, NY, NZ), jnp.float32) ** level_of(seeds[2], (LEVELS, NX, NY, NZ), ((1, 4), (2, 4), (3, 2)), -0.2, 0.2), 0.2, 1.0),
        "congestion": jnp.clip(0.5 + 1.0 * jax.random.uniform(seeds[3], (LEVELS, NX, NY, NZ), jnp.float32) ** level_of(seeds[3], (LEVELS, NX, NY, NZ), ((1, 4), (2, 4), (3, 2)), -0.2, 0.2), 0.5, 1.5),
    }


time_rate = 1.0

def minus_laplace(field):
    padded = jnp.pad(field, ((0, 0), (0, 0), (1, 1), (1, 1), (1, 1)))
    center = padded[:, :, 1:-1, 1:-1, 1:-1]
    beside = padded[:, :, 2:, 1:-1, 1:-1] + padded[:, :, :-2, 1:-1, 1:-1]
    beside = beside + padded[:, :, 1:-1, 2:, 1:-1] + padded[:, :, 1:-1, :-2, 1:-1]
    beside = beside + padded[:, :, 1:-1, 1:-1, 2:] + padded[:, :, 1:-1, 1:-1, :-2]
    return 6.0 * center - beside

def jacobian(vector, lapped, reaction, transport, congestion):
    value_part, density_part = (vector[0], vector[1])
    later = jnp.concatenate([value_part[1:], jnp.zeros_like(value_part[:1])], 0)
    earlier = jnp.concatenate([jnp.zeros_like(density_part[:1]), density_part[:-1]], 0)
    first = time_rate * (value_part - later) + lapped[0] + reaction * value_part - congestion * density_part
    second = time_rate * (density_part - earlier) + lapped[1] + reaction * density_part - transport * lapped[0]
    return jnp.stack([first, second], 0)

def precondition(vector, reaction, transport):
    levels = vector.shape[1]
    diag = time_rate + 6.0 + reaction
    value_levels = [None] * levels
    carry = jnp.zeros_like(vector[0, 0])
    for level in range(levels - 1, -1, -1):
        carry = (vector[0, level] + time_rate * carry) / diag[level]
        value_levels[level] = carry
    density_levels = []
    carry = jnp.zeros_like(vector[1, 0])
    for level in range(levels):
        carry = (vector[1, level] + time_rate * carry + 6.0 * transport[level] * value_levels[level]) / diag[level]
        density_levels.append(carry)
    return jnp.stack([jnp.stack(value_levels, 0), jnp.stack(density_levels, 0)], 0)

def least_squares(columns, beta, steps):
    rotations = []
    target = [beta] + [jnp.float32(0.0)] * steps
    upper = []
    for column_index in range(steps):
        column = list(columns[column_index])
        for place, (cosine, sine) in enumerate(rotations):
            upper_entry = cosine * column[place] + sine * column[place + 1]
            lower_entry = -sine * column[place] + cosine * column[place + 1]
            column[place], column[place + 1] = (upper_entry, lower_entry)
        radius = jnp.sqrt(column[column_index] ** 2 + column[column_index + 1] ** 2)
        cosine = column[column_index] / radius
        sine = column[column_index + 1] / radius
        column[column_index] = radius
        rotations.append((cosine, sine))
        target[column_index], target[column_index + 1] = (cosine * target[column_index], -sine * target[column_index])
        upper.append(column[:column_index + 1])
    solved = [None] * steps
    for row_index in range(steps - 1, -1, -1):
        accum = target[row_index]
        for later_index in range(row_index + 1, steps):
            accum = accum - upper[later_index][row_index] * solved[later_index]
        solved[row_index] = accum / upper[row_index][row_index]
    return solved

def reference(residual_in, reaction, transport, congestion):
    beta = jnp.sqrt(jnp.sum(residual_in * residual_in))
    basis = [residual_in / beta]
    columns = []
    for column_index in range(ITERS):
        search = precondition(basis[column_index], reaction, transport)
        image = jacobian(search, minus_laplace(search), reaction, transport, congestion)
        coeffs = [jnp.sum(vector * image) for vector in basis]
        for coeff, vector in zip(coeffs, basis):
            image = image - coeff * vector
        height = jnp.sqrt(jnp.sum(image * image))
        basis.append(image / height)
        columns.append(coeffs + [height])
    solved = least_squares(columns, beta, ITERS)
    update = jnp.zeros_like(residual_in)
    for column_index in range(ITERS):
        update = update + solved[column_index] * precondition(basis[column_index], reaction, transport)
    return update
```

```python
import functools

import jax
import jax.numpy as jnp
from jax import lax
from jax.experimental import pallas as pl
from jax.experimental.pallas import tpu as pltpu
from jax.sharding import PartitionSpec as P

ITERS = 8
AXES = ("gx", "gy", "gz")
time_rate = 1.0
SCALE = 2.5
BACK = 1.0
PIVOT = 2.5e-3


def pair_index(row, column):
    return column * (column + 1) // 2 + row


def least_squares(columns, beta, steps):
    zero = jnp.zeros_like(beta)
    rotations = []
    target = [beta] + [zero] * steps
    upper = []
    for column_index in range(steps):
        column = list(columns[column_index])
        for place, (cosine, sine) in enumerate(rotations):
            upper_entry = cosine * column[place] + sine * column[place + 1]
            lower_entry = -sine * column[place] + cosine * column[place + 1]
            column[place], column[place + 1] = (upper_entry, lower_entry)
        radius = jnp.sqrt(column[column_index] ** 2 + column[column_index + 1] ** 2)
        inverse = 1.0 / radius
        cosine = column[column_index] * inverse
        sine = column[column_index + 1] * inverse
        column[column_index] = inverse
        rotations.append((cosine, sine))
        target[column_index], target[column_index + 1] = (
            cosine * target[column_index],
            -sine * target[column_index],
        )
        upper.append(column[: column_index + 1])
    solved = [None] * steps
    for row_index in range(steps - 1, -1, -1):
        accum = target[row_index]
        for later_index in range(steps - 1, row_index, -1):
            accum = accum - upper[later_index][row_index] * solved[later_index]
        solved[row_index] = accum * upper[row_index][row_index]
    return solved


def gram_solve(gram, steps):
    size = steps + 1
    work = {(i, j): gram(i, j) for j in range(size) for i in range(j + 1)}
    factor = {}
    worst = None
    for i in range(size):
        ratio = work[i, i] / gram(i, i)
        worst = ratio if worst is None else jnp.where(ratio > worst, worst, ratio)
        pivot = jnp.sqrt(work[i, i])
        inverse = 1.0 / pivot
        factor[i, i] = pivot
        for j in range(i + 1, size):
            factor[i, j] = work[i, j] * inverse
        for a in range(i + 1, size):
            for b in range(a, size):
                work[a, b] = work[a, b] - factor[i, a] * factor[i, b]
    columns = []
    for k in range(steps):
        column = []
        for i in range(k + 2):
            entry = -factor[i, k + 1] * (1.0 / SCALE)
            if i <= k:
                entry = entry + factor[i, k]
            if k > 0 and i <= k - 1:
                entry = entry - factor[i, k - 1] * (BACK / SCALE)
            column.append(entry)
        columns.append(column)
    return least_squares(columns, factor[0, 0], steps), worst


def kernel(
    levels, sizes, residual, reaction, transport, congestion, out, flag,
    basis, inv, weight, couple, search, xin, yout, yin, zout, zin,
    gram, splat, gsend, gall, insem, ssem, rsem, gssem, grsem,
):
    fields = 2 * levels
    nx, ny, nz = residual.shape[1:]
    total = sizes[0] * sizes[1] * sizes[2]
    index = [lax.axis_index(axis) for axis in AXES]
    me = (index[0] * sizes[1] + index[1]) * sizes[2] + index[2]
    lane = lax.broadcasted_iota(jnp.int32, (ny, nz), 1)
    sub = lax.broadcasted_iota(jnp.int32, (ny, nz), 0)

    loads = [
        pltpu.make_async_copy(src, dst, insem.at[place])
        for place, (src, dst) in enumerate(
            ((residual, basis.at[0]), (reaction, inv), (transport, weight), (congestion, couple))
        )
    ]
    for load in loads:
        load.start()

    for buffer in (xin, yin, zin):
        buffer[...] = jnp.zeros_like(buffer)
    gram[...] = jnp.zeros_like(gram)

    def ident(other):
        return (other // (sizes[1] * sizes[2]), (other // sizes[2]) % sizes[1], other % sizes[2])

    barrier = pltpu.get_barrier_semaphore()

    def greet(step, carry):
        pl.semaphore_signal(
            barrier, inc=1, device_id=ident((me + step) % total),
            device_id_type=pl.DeviceIdType.MESH,
        )
        return carry

    lax.fori_loop(1, total, greet, 0)

    def remote(axis, side, slot):
        if axis == 0:
            src, dst = search.at[slot, :, nx - 1 if side == 0 else 0], xin.at[slot, side]
        elif axis == 1:
            src, dst = yout.at[slot, side], yin.at[slot, side]
        else:
            src, dst = zout.at[slot, side], zin.at[slot, side]
        target = list(index)
        target[axis] = index[axis] + (1 if side == 0 else -1)
        return pltpu.make_async_remote_copy(
            src_ref=src, dst_ref=dst,
            send_sem=ssem.at[axis, side, slot], recv_sem=rsem.at[axis, side, slot],
            device_id=tuple(target), device_id_type=pl.DeviceIdType.MESH,
        )

    def sends(axis, side):
        return index[axis] < sizes[axis] - 1 if side == 0 else index[axis] > 0

    def receives(axis, side):
        return index[axis] > 0 if side == 0 else index[axis] < sizes[axis] - 1

    def start(axis, slot):
        odd = index[axis] % 2 == 1
        up, down = sends(axis, 0), sends(axis, 1)

        @pl.when(jnp.logical_and(odd, up))
        def _():
            remote(axis, 0, slot).start()

        @pl.when(down)
        def _():
            remote(axis, 1, slot).start()

        @pl.when(jnp.logical_and(jnp.logical_not(odd), up))
        def _():
            remote(axis, 0, slot).start()

    def wait_sent(axis, slot):
        for side in range(2):
            @pl.when(sends(axis, side))
            def _():
                remote(axis, side, slot).wait_send()

    def wait_received(axis, slot):
        for side in range(2):
            @pl.when(receives(axis, side))
            def _():
                remote(axis, side, slot).wait_recv()

    def precondition(x, vector):
        value, density = [None] * levels, [None] * levels
        carry = None
        for t in range(levels - 1, -1, -1):
            carry = vector[t] if carry is None else vector[t] + carry
            carry = carry * inv[t, x]
            value[t] = carry
        carry = None
        for t in range(levels):
            push = vector[levels + t] + (6.0 * weight[t, x]) * value[t]
            carry = push if carry is None else push + carry
            carry = carry * inv[t, x]
            density[t] = carry
        return value + density

    def publish(x, vector, slot, packs):
        high, low = packs
        found = precondition(x, vector)
        for f in range(fields):
            item = found[f]
            search[slot, f, x] = item
            yout[slot, 0, f, pl.ds(x, 1), :] = item[ny - 1 : ny, :]
            yout[slot, 1, f, pl.ds(x, 1), :] = item[0:1, :]
            place = x * fields + f
            turned = pltpu.roll(item, place, 1)
            high = jnp.where(lane == (place + nz - 1) % nz, turned, high)
            low = jnp.where(lane == place, turned, low)
        return high, low

    def advance(x, k, slot, xlow, xhigh):
        sums, centers = [], []
        zlow, zhigh = zin[slot, 0], zin[slot, 1]
        for f in range(fields):
            center = search[slot, f, x]
            up = jnp.where(sub == 0, yin[slot, 0, f, pl.ds(x, 1), :], pltpu.roll(center, 1, 0))
            down = jnp.where(
                sub == ny - 1, yin[slot, 1, f, pl.ds(x, 1), :], pltpu.roll(center, ny - 1, 0)
            )
            place = x * fields + f
            edge = jnp.where(lane == (place + nz - 1) % nz, zlow, zhigh)
            edge = pltpu.roll(edge, (nz - place) % nz, 1)
            left = pltpu.roll(jnp.where(lane == nz - 1, edge, center), 1, 1)
            right = pltpu.roll(jnp.where(lane == 0, edge, center), nz - 1, 1)
            sums.append(((xlow(f) + xhigh(f)) + (up + down)) + (left + right))
            centers.append(center)
        result = [None] * fields
        for t in range(levels):
            result[t] = sums[t] + couple[t, x] * centers[levels + t]
            result[levels + t] = sums[levels + t] - weight[t, x] * sums[t]
        for f in range(fields):
            item = SCALE * result[f]
            if k > 0:
                item = item - BACK * basis[k - 1, f, x]
            basis[k + 1, f, x] = item
            result[f] = item
        return result

    def dots(k):
        def step(x, accs):
            accs = list(accs)
            for f in range(fields):
                own = basis[k, f, x]
                for j in range(k + 1):
                    other = own if j == k else basis[j, f, x]
                    accs[j] = accs[j] + own * other
            return tuple(accs)

        zero = jnp.zeros((ny, nz), jnp.float32)
        accs = lax.fori_loop(0, nx, step, (zero,) * (k + 1))
        for j in range(k + 1):
            row = pair_index(j, k)
            gram[row : row + 1, :] = jnp.sum(accs[j], axis=0, keepdims=True)

    for load in loads:
        load.wait()

    def invert(x, carry):
        for t in range(levels):
            inv[t, x] = 1.0 / (time_rate + 6.0 + inv[t, x])
        return carry

    lax.fori_loop(0, nx, invert, 0)
    blank = jnp.zeros((ny, nz), jnp.float32)

    def first(x, packs):
        return publish(x, [basis[0, f, x] for f in range(fields)], 0, packs)

    packs = lax.fori_loop(0, nx, first, (blank, blank))
    zout[0, 0], zout[0, 1] = packs
    pl.semaphore_wait(barrier, total - 1)
    start(0, 0)
    start(1, 0)
    start(2, 0)

    for k in range(ITERS):
        slot, later = k % 2, (k + 1) % 2
        last = k == ITERS - 1
        dots(k)
        if k > 0:
            for axis in range(3):
                wait_sent(axis, later)
        wait_received(2, slot)
        wait_received(1, slot)

        def inner(x, packs):
            vector = advance(
                x, k, slot, lambda f: search[slot, f, x - 1], lambda f: search[slot, f, x + 1]
            )
            return packs if last else publish(x, vector, later, packs)

        packs = lax.fori_loop(1, nx - 1, inner, (blank, blank))
        wait_received(0, slot)
        bottom = advance(0, k, slot, lambda f: xin[slot, 0, f], lambda f: search[slot, f, 1])
        if not last:
            packs = publish(0, bottom, later, packs)
        top = advance(
            nx - 1, k, slot, lambda f: search[slot, f, nx - 2], lambda f: xin[slot, 1, f]
        )
        if not last:
            packs = publish(nx - 1, top, later, packs)
            zout[later, 0], zout[later, 1] = packs
            for axis in range(3):
                start(axis, later)

    dots(ITERS)
    for axis in range(3):
        wait_sent(axis, (ITERS - 1) % 2)

    local = jnp.sum(gram[...].T, axis=0, keepdims=True)
    gsend[...] = local
    gall[me] = local

    def spread(step, carry):
        pltpu.make_async_remote_copy(
            src_ref=gsend, dst_ref=gall.at[me], send_sem=gssem, recv_sem=grsem,
            device_id=ident((me + step) % total), device_id_type=pl.DeviceIdType.MESH,
        ).start()
        return carry

    lax.fori_loop(1, total, spread, 0)
    others = gall.at[pl.ds(0, total - 1)]
    pltpu.make_async_copy(others, others, grsem).wait()
    pltpu.make_async_copy(others, others, gssem).wait()
    whole = jnp.sum(gall[...], axis=0)
    splat[...] = jnp.broadcast_to(whole, splat.shape).T

    def entry(i, j):
        row = pair_index(i, j)
        return splat[row : row + 1, :]

    solved, worst = gram_solve(entry, ITERS)
    flag[...] = jnp.broadcast_to(worst, flag.shape)

    def combine(x, carry):
        vector = []
        for f in range(fields):
            item = solved[0] * basis[0, f, x]
            for k in range(1, ITERS):
                item = item + solved[k] * basis[k, f, x]
            vector.append(item)
        found = precondition(x, vector)
        for f in range(fields):
            out[f, x] = found[f]
        return carry

    lax.fori_loop(0, nx, combine, 0)


def fused(sizes, residual, reaction, transport, congestion):
    levels, nx, ny, nz = reaction.shape
    fields = 2 * levels
    total = sizes[0] * sizes[1] * sizes[2]
    pairs = pair_index(ITERS, ITERS) + 1
    assert fields * nx <= nz and pairs <= nz
    f32 = jnp.float32
    hbm = pl.BlockSpec(memory_space=pl.ANY)
    vmem = pl.BlockSpec(memory_space=pltpu.VMEM)
    out, flag = pl.pallas_call(
        functools.partial(kernel, levels, sizes),
        out_shape=(
            jax.ShapeDtypeStruct((fields, nx, ny, nz), f32),
            jax.ShapeDtypeStruct((8, nz), f32),
        ),
        in_specs=[hbm] * 4,
        out_specs=(vmem, vmem),
        scratch_shapes=[
            pltpu.VMEM((ITERS + 1, fields, nx, ny, nz), f32),
            pltpu.VMEM((levels, nx, ny, nz), f32),
            pltpu.VMEM((levels, nx, ny, nz), f32),
            pltpu.VMEM((levels, nx, ny, nz), f32),
            pltpu.VMEM((2, fields, nx, ny, nz), f32),
            pltpu.VMEM((2, 2, fields, ny, nz), f32),
            pltpu.VMEM((2, 2, fields, nx, nz), f32),
            pltpu.VMEM((2, 2, fields, nx, nz), f32),
            pltpu.VMEM((2, 2, ny, nz), f32),
            pltpu.VMEM((2, 2, ny, nz), f32),
            pltpu.VMEM((nz, nz), f32),
            pltpu.VMEM((nz, nz), f32),
            pltpu.VMEM((1, nz), f32),
            pltpu.VMEM((total, 1, nz), f32),
            pltpu.SemaphoreType.DMA((4,)),
            pltpu.SemaphoreType.DMA((3, 2, 2)),
            pltpu.SemaphoreType.DMA((3, 2, 2)),
            pltpu.SemaphoreType.DMA,
            pltpu.SemaphoreType.DMA,
        ],
        compiler_params=pltpu.CompilerParams(
            collective_id=0, has_side_effects=True, vmem_limit_bytes=40 * 1024 * 1024
        ),
        name="krylov",
    )(residual.reshape((fields, nx, ny, nz)), reaction, transport, congestion)
    return out.reshape(residual.shape), flag


def neighbours(field):
    total = 0.0
    for axis, dim in (("gx", 2), ("gy", 3), ("gz", 4)):
        count = lax.axis_size(axis)
        size = field.shape[dim]
        forward = [(i, i + 1) for i in range(count - 1)]
        backward = [(target, source) for source, target in forward]
        low = lax.ppermute(lax.slice_in_dim(field, size - 1, size, axis=dim), axis, forward)
        high = lax.ppermute(lax.slice_in_dim(field, 0, 1, axis=dim), axis, backward)
        below = jnp.concatenate([low, lax.slice_in_dim(field, 0, size - 1, axis=dim)], dim)
        above = jnp.concatenate([lax.slice_in_dim(field, 1, size, axis=dim), high], dim)
        total = total + below + above
    return total


def jacobian(vector, reaction, transport, congestion):
    lapped = 6.0 * vector - neighbours(vector)
    value_part, density_part = (vector[0], vector[1])
    later = jnp.concatenate([value_part[1:], jnp.zeros_like(value_part[:1])], 0)
    earlier = jnp.concatenate([jnp.zeros_like(density_part[:1]), density_part[:-1]], 0)
    first = (
        time_rate * (value_part - later)
        + lapped[0]
        + reaction * value_part
        - congestion * density_part
    )
    second = (
        time_rate * (density_part - earlier)
        + lapped[1]
        + reaction * density_part
        - transport * lapped[0]
    )
    return jnp.stack([first, second], 0)


def precondition(vector, reaction, transport):
    levels = vector.shape[1]
    diag = time_rate + 6.0 + reaction
    value_levels = [None] * levels
    carry = jnp.zeros_like(vector[0, 0])
    for level in range(levels - 1, -1, -1):
        carry = (vector[0, level] + time_rate * carry) / diag[level]
        value_levels[level] = carry
    density_levels = []
    carry = jnp.zeros_like(vector[1, 0])
    for level in range(levels):
        carry = (
            vector[1, level] + time_rate * carry + 6.0 * transport[level] * value_levels[level]
        ) / diag[level]
        density_levels.append(carry)
    return jnp.stack([jnp.stack(value_levels, 0), jnp.stack(density_levels, 0)], 0)


def arnoldi(residual, reaction, transport, congestion):
    dims = tuple(range(1, residual.ndim + 1))
    beta = jnp.sqrt(lax.psum(jnp.sum(residual * residual), AXES))
    basis = jnp.zeros((ITERS + 1,) + residual.shape, residual.dtype).at[0].set(residual / beta)
    heights = jnp.zeros((ITERS, ITERS + 1), residual.dtype)

    def step(c, state):
        basis, heights = state
        search = precondition(basis[c], reaction, transport)
        image = jacobian(search, reaction, transport, congestion)
        coeffs = lax.psum(jnp.sum(basis * image[None], axis=dims), AXES)
        image = image - jnp.sum(coeffs.reshape((-1,) + (1,) * residual.ndim) * basis, axis=0)
        height = jnp.sqrt(lax.psum(jnp.sum(image * image), AXES))
        basis = basis.at[c + 1].set(image / height)
        return basis, heights.at[c].set(coeffs.at[c + 1].set(height))

    basis, heights = lax.fori_loop(0, ITERS, step, (basis, heights))
    columns = [[heights[c, i] for i in range(c + 2)] for c in range(ITERS)]
    solved = least_squares(columns, beta, ITERS)
    mixed = sum(solved[c] * basis[c] for c in range(ITERS))
    return precondition(mixed, reaction, transport)


def body(sizes, residual_in, reaction, transport, congestion):
    update, flag = fused(sizes, residual_in, reaction, transport, congestion)
    return lax.cond(
        flag[0, 0] > PIVOT,
        lambda update, *rest: update,
        lambda update, *rest: arnoldi(*rest),
        update, residual_in, reaction, transport, congestion,
    )


def solution(mesh):
    placed = (
        P(None, None, "gx", "gy", "gz"),
        P(None, "gx", "gy", "gz"),
        P(None, "gx", "gy", "gz"),
        P(None, "gx", "gy", "gz"),
    )
    sizes = tuple(mesh.shape[axis] for axis in AXES)
    return jax.shard_map(
        functools.partial(body, sizes), mesh=mesh, in_specs=placed,
        out_specs=P(None, None, "gx", "gy", "gz"), check_vma=False,
    )
```

```python
import functools

import jax
import jax.numpy as jnp
from jax import lax
from jax.experimental import pallas as pl
from jax.experimental.pallas import tpu as pltpu
from jax.sharding import PartitionSpec as P

ITERS = 8
AXES = ("gx", "gy", "gz")
time_rate = 1.0
SCALE = 2.5
BACK = 1.0
PIVOT = 2.5e-3
PLANES = 2


def pair_index(row, column):
    return column * (column + 1) // 2 + row


def least_squares(columns, beta, steps):
    zero = jnp.zeros_like(beta)
    rotations = []
    target = [beta] + [zero] * steps
    upper = []
    for column_index in range(steps):
        column = list(columns[column_index])
        for place, (cosine, sine) in enumerate(rotations):
            upper_entry = cosine * column[place] + sine * column[place + 1]
            lower_entry = -sine * column[place] + cosine * column[place + 1]
            column[place], column[place + 1] = (upper_entry, lower_entry)
        radius = jnp.sqrt(column[column_index] ** 2 + column[column_index + 1] ** 2)
        inverse = 1.0 / radius
        cosine = column[column_index] * inverse
        sine = column[column_index + 1] * inverse
        column[column_index] = inverse
        rotations.append((cosine, sine))
        target[column_index], target[column_index + 1] = (
            cosine * target[column_index],
            -sine * target[column_index],
        )
        upper.append(column[: column_index + 1])
    solved = [None] * steps
    for row_index in range(steps - 1, -1, -1):
        accum = target[row_index]
        for later_index in range(steps - 1, row_index, -1):
            accum = accum - upper[later_index][row_index] * solved[later_index]
        solved[row_index] = accum * upper[row_index][row_index]
    return solved


def gram_solve(gram, steps):
    size = steps + 1
    work = {(i, j): gram(i, j) for j in range(size) for i in range(j + 1)}
    factor = {}
    worst = None
    for i in range(size):
        ratio = work[i, i] / gram(i, i)
        worst = ratio if worst is None else jnp.where(ratio > worst, worst, ratio)
        pivot = jnp.sqrt(work[i, i])
        inverse = 1.0 / pivot
        factor[i, i] = pivot
        for j in range(i + 1, size):
            factor[i, j] = work[i, j] * inverse
        for a in range(i + 1, size):
            for b in range(a, size):
                work[a, b] = work[a, b] - factor[i, a] * factor[i, b]
    columns = []
    for k in range(steps):
        column = []
        for i in range(k + 2):
            entry = -factor[i, k + 1] * (1.0 / SCALE)
            if i <= k:
                entry = entry + factor[i, k]
            if k > 0 and i <= k - 1:
                entry = entry - factor[i, k - 1] * (BACK / SCALE)
            column.append(entry)
        columns.append(column)
    return least_squares(columns, factor[0, 0], steps), worst


def kernel(
    levels, sizes, residual, reaction, transport, congestion, out, flag,
    basis, inv, weight, couple, search, xin, yout, yin, zout, zin,
    gram, splat, gsend, gall, insem, ssem, rsem, gssem, grsem,
):
    fields = 2 * levels
    nx, ny, nz = residual.shape[1:]
    total = sizes[0] * sizes[1] * sizes[2]
    index = [lax.axis_index(axis) for axis in AXES]
    me = (index[0] * sizes[1] + index[1]) * sizes[2] + index[2]
    lane = lax.broadcasted_iota(jnp.int32, (ny, nz), 1)
    sub = lax.broadcasted_iota(jnp.int32, (ny, nz), 0)

    loads = [
        pltpu.make_async_copy(src, dst, insem.at[place])
        for place, (src, dst) in enumerate(
            ((residual, basis.at[0]), (reaction, inv), (transport, weight), (congestion, couple))
        )
    ]
    for load in loads:
        load.start()

    for buffer in (xin, yin, zin):
        buffer[...] = jnp.zeros_like(buffer)
    gram[...] = jnp.zeros_like(gram)

    def ident(other):
        return (other // (sizes[1] * sizes[2]), (other // sizes[2]) % sizes[1], other % sizes[2])

    barrier = pltpu.get_barrier_semaphore()

    def greet(step, carry):
        pl.semaphore_signal(
            barrier, inc=1, device_id=ident((me + step) % total),
            device_id_type=pl.DeviceIdType.MESH,
        )
        return carry

    lax.fori_loop(1, total, greet, 0)

    def remote(axis, side, slot):
        if axis == 0:
            src, dst = search.at[slot, :, nx - 1 if side == 0 else 0], xin.at[slot, side]
        elif axis == 1:
            src, dst = yout.at[slot, side], yin.at[slot, side]
        else:
            src, dst = zout.at[slot, side], zin.at[slot, side]
        target = list(index)
        target[axis] = index[axis] + (1 if side == 0 else -1)
        return pltpu.make_async_remote_copy(
            src_ref=src, dst_ref=dst,
            send_sem=ssem.at[axis, side, slot], recv_sem=rsem.at[axis, side, slot],
            device_id=tuple(target), device_id_type=pl.DeviceIdType.MESH,
        )

    def sends(axis, side):
        return index[axis] < sizes[axis] - 1 if side == 0 else index[axis] > 0

    def receives(axis, side):
        return index[axis] > 0 if side == 0 else index[axis] < sizes[axis] - 1

    def start(axis, slot):
        odd = index[axis] % 2 == 1
        up, down = sends(axis, 0), sends(axis, 1)

        @pl.when(jnp.logical_and(odd, up))
        def _():
            remote(axis, 0, slot).start()

        @pl.when(down)
        def _():
            remote(axis, 1, slot).start()

        @pl.when(jnp.logical_and(jnp.logical_not(odd), up))
        def _():
            remote(axis, 0, slot).start()

    def wait_sent(axis, slot):
        for side in range(2):
            @pl.when(sends(axis, side))
            def _():
                remote(axis, side, slot).wait_send()

    def wait_received(axis, slot):
        for side in range(2):
            @pl.when(receives(axis, side))
            def _():
                remote(axis, side, slot).wait_recv()

    def precondition(x, vector):
        value, density = [None] * levels, [None] * levels
        carry = None
        for t in range(levels - 1, -1, -1):
            carry = vector[t] if carry is None else vector[t] + carry
            carry = carry * inv[t, x]
            value[t] = carry
        carry = None
        for t in range(levels):
            push = vector[levels + t] + (6.0 * weight[t, x]) * value[t]
            carry = push if carry is None else push + carry
            carry = carry * inv[t, x]
            density[t] = carry
        return value + density

    def publish(planes, vectors, slot, packs):
        high, low = packs
        founds = [precondition(x, vector) for x, vector in zip(planes, vectors)]
        for x, found in zip(planes, founds):
            for f in range(fields):
                place = x * fields + f
                turned = pltpu.roll(found[f], place, 1)
                high = jnp.where(lane == (place + nz - 1) % nz, turned, high)
                low = jnp.where(lane == place, turned, low)
        for x, found in zip(planes, founds):
            for f in range(fields):
                search[slot, f, x] = found[f]
                yout[slot, 0, f, pl.ds(x, 1), :] = found[f][ny - 1 : ny, :]
                yout[slot, 1, f, pl.ds(x, 1), :] = found[f][0:1, :]
        return high, low

    def spatial(k, slot, planes):
        founds = [spatial_plane(k, slot, *plane) for plane in planes]
        for (x, _, _), found in zip(planes, founds):
            for f in range(fields):
                basis[k + 1, f, x] = found[f]

    def spatial_plane(k, slot, x, xlow, xhigh):
        def around(f):
            center = search[slot, f, x]
            up = jnp.where(sub == 0, 0.0, pltpu.roll(center, 1, 0))
            down = jnp.where(sub == ny - 1, 0.0, pltpu.roll(center, ny - 1, 0))
            place = x * fields + f
            edge = jnp.where(lane == (place + nz - 1) % nz, zin[slot, 0], zin[slot, 1])
            edge = pltpu.roll(edge, (nz - place) % nz, 1)
            left = pltpu.roll(jnp.where(lane == nz - 1, edge, center), 1, 1)
            right = pltpu.roll(jnp.where(lane == 0, edge, center), nz - 1, 1)
            return ((xlow(f) + xhigh(f)) + (up + down)) + (left + right)

        found = [None] * fields
        for t in range(levels):
            value = around(t)
            density = around(levels + t) - weight[t, x] * value
            value = value + couple[t, x] * search[slot, levels + t, x]
            for f, item in ((t, value), (levels + t, density)):
                item = SCALE * item
                if k > 0:
                    item = item - BACK * basis[k - 1, f, x]
                found[f] = item
        return found

    def finish(x, k, slot):
        def rows(f):
            low, high = yin[slot, 0, f, pl.ds(x, 1), :], yin[slot, 1, f, pl.ds(x, 1), :]
            return SCALE * jnp.where(sub == 0, low, jnp.where(sub == ny - 1, high, 0.0))

        vector = [None] * fields
        for t in range(levels - 1, -1, -1):
            value = rows(t)
            density = rows(levels + t) - weight[t, x] * value
            for f, item in ((t, value), (levels + t, density)):
                vector[f] = basis[k + 1, f, x] + item
        return vector

    def dots(k):
        def step(x, accs):
            accs = list(accs)
            for f in range(fields):
                own = basis[k, f, x]
                for j in range(k + 1):
                    other = own if j == k else basis[j, f, x]
                    accs[j] = accs[j] + own * other
            return tuple(accs)

        zero = jnp.zeros((ny, nz), jnp.float32)
        accs = lax.fori_loop(0, nx, step, (zero,) * (k + 1))
        for j in range(k + 1):
            row = pair_index(j, k)
            gram[row : row + 1, :] = jnp.sum(accs[j], axis=0, keepdims=True)

    for load in loads:
        load.wait()

    def invert(x, carry):
        for t in range(levels):
            inv[t, x] = 1.0 / (time_rate + 6.0 + inv[t, x])
        return carry

    lax.fori_loop(0, nx, invert, 0)
    blank = jnp.zeros((ny, nz), jnp.float32)

    def first(x, packs):
        planes = [x * PLANES + place for place in range(PLANES)]
        vectors = [[basis[0, f, x] for f in range(fields)] for x in planes]
        return publish(planes, vectors, 0, packs)

    packs = lax.fori_loop(0, nx // PLANES, first, (blank, blank))
    zout[0, 0], zout[0, 1] = packs
    pl.semaphore_wait(barrier, total - 1)
    start(0, 0)
    start(1, 0)
    start(2, 0)

    for k in range(ITERS):
        slot, later = k % 2, (k + 1) % 2
        last = k == ITERS - 1
        dots(k)
        if k > 0:
            for axis in range(3):
                wait_sent(axis, later)
        wait_received(2, slot)

        def inner(step, carry):
            spatial(k, slot, [
                (
                    x,
                    lambda f, x=x: search[slot, f, x - 1],
                    lambda f, x=x: search[slot, f, x + 1],
                )
                for x in (1 + step * PLANES + place for place in range(PLANES))
            ])
            return carry

        lax.fori_loop(0, (nx - 2) // PLANES, inner, 0)
        wait_received(1, slot)

        def settle(planes, packs):
            vectors = [finish(x, k, slot) for x in planes]
            for x, vector in zip(planes, vectors):
                for f in range(fields):
                    basis[k + 1, f, x] = vector[f]
            return packs if last else publish(planes, vectors, later, packs)

        packs = lax.fori_loop(
            0, (nx - 2) // PLANES,
            lambda step, packs: settle(
                [1 + step * PLANES + place for place in range(PLANES)], packs
            ),
            (blank, blank),
        )
        wait_received(0, slot)
        spatial(k, slot, [
            (0, lambda f: xin[slot, 0, f], lambda f: search[slot, f, 1]),
            (nx - 1, lambda f: search[slot, f, nx - 2], lambda f: xin[slot, 1, f]),
        ])
        packs = settle([0, nx - 1], packs)
        if not last:
            zout[later, 0], zout[later, 1] = packs
            for axis in range(3):
                start(axis, later)

    dots(ITERS)
    for axis in range(3):
        wait_sent(axis, (ITERS - 1) % 2)

    local = jnp.sum(gram[...].T, axis=0, keepdims=True)
    gsend[...] = local
    gall[me] = local

    def spread(step, carry):
        pltpu.make_async_remote_copy(
            src_ref=gsend, dst_ref=gall.at[me], send_sem=gssem, recv_sem=grsem,
            device_id=ident((me + step) % total), device_id_type=pl.DeviceIdType.MESH,
        ).start()
        return carry

    lax.fori_loop(1, total, spread, 0)
    others = gall.at[pl.ds(0, total - 1)]
    pltpu.make_async_copy(others, others, grsem).wait()
    pltpu.make_async_copy(others, others, gssem).wait()
    whole = jnp.sum(gall[...], axis=0)
    splat[...] = jnp.broadcast_to(whole, splat.shape).T

    def entry(i, j):
        row = pair_index(i, j)
        return splat[row : row + 1, :]

    solved, worst = gram_solve(entry, ITERS)
    flag[...] = jnp.broadcast_to(worst, flag.shape)

    def combine(x, carry):
        vector = []
        for f in range(fields):
            item = solved[0] * basis[0, f, x]
            for k in range(1, ITERS):
                item = item + solved[k] * basis[k, f, x]
            vector.append(item)
        found = precondition(x, vector)
        for f in range(fields):
            out[f, x] = found[f]
        return carry

    lax.fori_loop(0, nx, combine, 0)


def fused(sizes, residual, reaction, transport, congestion):
    levels, nx, ny, nz = reaction.shape
    fields = 2 * levels
    total = sizes[0] * sizes[1] * sizes[2]
    pairs = pair_index(ITERS, ITERS) + 1
    assert fields * nx <= nz and pairs <= nz and nx % PLANES == 0
    f32 = jnp.float32
    hbm = pl.BlockSpec(memory_space=pl.ANY)
    vmem = pl.BlockSpec(memory_space=pltpu.VMEM)
    out, flag = pl.pallas_call(
        functools.partial(kernel, levels, sizes),
        out_shape=(
            jax.ShapeDtypeStruct((fields, nx, ny, nz), f32),
            jax.ShapeDtypeStruct((8, nz), f32),
        ),
        in_specs=[hbm] * 4,
        out_specs=(vmem, vmem),
        scratch_shapes=[
            pltpu.VMEM((ITERS + 1, fields, nx, ny, nz), f32),
            pltpu.VMEM((levels, nx, ny, nz), f32),
            pltpu.VMEM((levels, nx, ny, nz), f32),
            pltpu.VMEM((levels, nx, ny, nz), f32),
            pltpu.VMEM((2, fields, nx, ny, nz), f32),
            pltpu.VMEM((2, 2, fields, ny, nz), f32),
            pltpu.VMEM((2, 2, fields, nx, nz), f32),
            pltpu.VMEM((2, 2, fields, nx, nz), f32),
            pltpu.VMEM((2, 2, ny, nz), f32),
            pltpu.VMEM((2, 2, ny, nz), f32),
            pltpu.VMEM((nz, nz), f32),
            pltpu.VMEM((nz, nz), f32),
            pltpu.VMEM((1, nz), f32),
            pltpu.VMEM((total, 1, nz), f32),
            pltpu.SemaphoreType.DMA((4,)),
            pltpu.SemaphoreType.DMA((3, 2, 2)),
            pltpu.SemaphoreType.DMA((3, 2, 2)),
            pltpu.SemaphoreType.DMA,
            pltpu.SemaphoreType.DMA,
        ],
        compiler_params=pltpu.CompilerParams(
            collective_id=0, has_side_effects=True, vmem_limit_bytes=40 * 1024 * 1024
        ),
        name="krylov",
    )(residual.reshape((fields, nx, ny, nz)), reaction, transport, congestion)
    return out.reshape(residual.shape), flag


def neighbours(field):
    total = 0.0
    for axis, dim in (("gx", 2), ("gy", 3), ("gz", 4)):
        count = lax.axis_size(axis)
        size = field.shape[dim]
        forward = [(i, i + 1) for i in range(count - 1)]
        backward = [(target, source) for source, target in forward]
        low = lax.ppermute(lax.slice_in_dim(field, size - 1, size, axis=dim), axis, forward)
        high = lax.ppermute(lax.slice_in_dim(field, 0, 1, axis=dim), axis, backward)
        below = jnp.concatenate([low, lax.slice_in_dim(field, 0, size - 1, axis=dim)], dim)
        above = jnp.concatenate([lax.slice_in_dim(field, 1, size, axis=dim), high], dim)
        total = total + below + above
    return total


def jacobian(vector, reaction, transport, congestion):
    lapped = 6.0 * vector - neighbours(vector)
    value_part, density_part = (vector[0], vector[1])
    later = jnp.concatenate([value_part[1:], jnp.zeros_like(value_part[:1])], 0)
    earlier = jnp.concatenate([jnp.zeros_like(density_part[:1]), density_part[:-1]], 0)
    first = (
        time_rate * (value_part - later)
        + lapped[0]
        + reaction * value_part
        - congestion * density_part
    )
    second = (
        time_rate * (density_part - earlier)
        + lapped[1]
        + reaction * density_part
        - transport * lapped[0]
    )
    return jnp.stack([first, second], 0)


def precondition(vector, reaction, transport):
    levels = vector.shape[1]
    diag = time_rate + 6.0 + reaction
    value_levels = [None] * levels
    carry = jnp.zeros_like(vector[0, 0])
    for level in range(levels - 1, -1, -1):
        carry = (vector[0, level] + time_rate * carry) / diag[level]
        value_levels[level] = carry
    density_levels = []
    carry = jnp.zeros_like(vector[1, 0])
    for level in range(levels):
        carry = (
            vector[1, level] + time_rate * carry + 6.0 * transport[level] * value_levels[level]
        ) / diag[level]
        density_levels.append(carry)
    return jnp.stack([jnp.stack(value_levels, 0), jnp.stack(density_levels, 0)], 0)


def arnoldi(residual, reaction, transport, congestion):
    dims = tuple(range(1, residual.ndim + 1))
    beta = jnp.sqrt(lax.psum(jnp.sum(residual * residual), AXES))
    basis = jnp.zeros((ITERS + 1,) + residual.shape, residual.dtype).at[0].set(residual / beta)
    heights = jnp.zeros((ITERS, ITERS + 1), residual.dtype)

    def step(c, state):
        basis, heights = state
        search = precondition(basis[c], reaction, transport)
        image = jacobian(search, reaction, transport, congestion)
        coeffs = lax.psum(jnp.sum(basis * image[None], axis=dims), AXES)
        image = image - jnp.sum(coeffs.reshape((-1,) + (1,) * residual.ndim) * basis, axis=0)
        height = jnp.sqrt(lax.psum(jnp.sum(image * image), AXES))
        basis = basis.at[c + 1].set(image / height)
        return basis, heights.at[c].set(coeffs.at[c + 1].set(height))

    basis, heights = lax.fori_loop(0, ITERS, step, (basis, heights))
    columns = [[heights[c, i] for i in range(c + 2)] for c in range(ITERS)]
    solved = least_squares(columns, beta, ITERS)
    mixed = sum(solved[c] * basis[c] for c in range(ITERS))
    return precondition(mixed, reaction, transport)


def body(sizes, residual_in, reaction, transport, congestion):
    update, flag = fused(sizes, residual_in, reaction, transport, congestion)
    return lax.cond(
        flag[0, 0] > PIVOT,
        lambda update, *rest: update,
        lambda update, *rest: arnoldi(*rest),
        update, residual_in, reaction, transport, congestion,
    )


def solution(mesh):
    placed = (
        P(None, None, "gx", "gy", "gz"),
        P(None, "gx", "gy", "gz"),
        P(None, "gx", "gy", "gz"),
        P(None, "gx", "gy", "gz"),
    )
    sizes = tuple(mesh.shape[axis] for axis in AXES)
    return jax.shard_map(
        functools.partial(body, sizes), mesh=mesh, in_specs=placed,
        out_specs=P(None, None, "gx", "gy", "gz"), check_vma=False,
    )
```
